32 devices in a mesh: dp: 4 (over y, core), tp: 8 (over z, x).
Axes of the slice: x: 2, y: 2, z: 4, core: 2. Of those that a mesh axis runs over, the one named last changes fastest.
Arguments:
- tokens: bfloat16 [1024, 7168], P(('dp', 'tp')), may hold values from -6 to 6
- w_gate: bfloat16 [7168, 12288], P(None, 'tp'), may hold values from -0.0625 to 0.0625
- w_up: bfloat16 [7168, 12288], P(None, 'tp'), may hold values from -0.0625 to 0.0625
- w_down: bfloat16 [12288, 7168], P('tp'), may hold values from -0.0546875 to 0.0546875
- cotangent: bfloat16 [1024, 7168], P(('dp', 'tp')), may hold values from -6 to 6
Outputs:
- mixed: bfloat16 [1024, 7168], P(('dp', 'tp'))
- input_grad: bfloat16 [1024, 7168], P(('dp', 'tp'))
- gate_grad: float32 [7168, 12288], P('dp', 'tp')
- up_grad: float32 [7168, 12288], P('dp', 'tp')
- down_grad: float32 [12288, 7168], P('tp', 'dp')
The draws below stay inside these ranges and needn't reach their ends.
All inputs are finite; a program needn't handle non-finite values.
Results may differ from the reference program's by a relative error of at most 0.0049.
Values may be sent and summed in bfloat16 or wider, within the bound.
No kernel may reach another device: no remote copies, remote signals or barrier semaphores. Data moves between devices by JAX's collectives and lax.ppermute only.
A program may use at most 192 MiB of HBM per device.

```python
import jax
import jax.numpy as jnp

D = 7168
FF = 12288
TOKENS = 1024


def shard_levels(key, shape, cuts, low, largest):
    def one(dim, parts):
        steps = jax.random.uniform(jax.random.fold_in(jax.random.fold_in(key, 6), dim), (parts,), jnp.float32, low / len(cuts), largest / len(cuts))
        return jnp.repeat(jnp.exp(steps), shape[dim] // parts).reshape((-1,) + (1,) * (len(shape) - dim - 1))

    loudness = one(*cuts[0])
    for cut in cuts[1:]:
        loudness = loudness * one(*cut)
    return loudness


def gaussian(own_key, extent, scale, reach, cuts=(), held_as=jnp.bfloat16):
    loudness = shard_levels(own_key, extent, cuts, -0.22, 0.18) if cuts else 1.0
    drawn = jax.random.normal(own_key, extent, jnp.float32) * scale * loudness
    return jnp.minimum(jnp.maximum(drawn, -reach), reach).astype(held_as)


def setup_inputs(seed: int = 0) -> dict:
    arg_keys = jax.random.split(jax.random.key(seed), 6)
    return {
        "tokens": gaussian(arg_keys[0], (TOKENS, D), 1.0, 6.0, ((0, 32),)),
        "w_gate": gaussian(arg_keys[1], (D, FF), D ** -0.5, 0.0625, ((1, 8),)),
        "w_up": gaussian(arg_keys[2], (D, FF), D ** -0.5, 0.0625, ((1, 8),)),
        "w_down": gaussian(arg_keys[3], (FF, D), FF ** -0.5, 0.0546875, ((0, 8),)),
        "cotangent": gaussian(arg_keys[4], (TOKENS, D), 1.0, 6.0, ((0, 32),)),
    }


def reference(tokens, w_gate, w_up, w_down, cotangent):
    gate = jnp.dot(tokens, w_gate, preferred_element_type=jnp.float32)
    up = jnp.dot(tokens, w_up, preferred_element_type=jnp.float32)
    sig = jax.nn.sigmoid(gate)
    act = gate * sig
    hidden = (act * up).astype(jnp.bfloat16)
    mixed = jnp.dot(hidden, w_down, preferred_element_type=jnp.float32).astype(jnp.bfloat16)
    back = jnp.dot(cotangent, w_down.T, preferred_element_type=jnp.float32)
    dgate = (back * up * sig * (1.0 + gate * (1.0 - sig))).astype(jnp.bfloat16)
    dup = (back * act).astype(jnp.bfloat16)
    input_grad = (jnp.dot(dgate, w_gate.T, preferred_element_type=jnp.float32)
                  + jnp.dot(dup, w_up.T, preferred_element_type=jnp.float32)).astype(jnp.bfloat16)
    gate_grad = jnp.dot(tokens.T, dgate, preferred_element_type=jnp.float32)
    up_grad = jnp.dot(tokens.T, dup, preferred_element_type=jnp.float32)
    down_grad = jnp.dot(hidden.T, cotangent, preferred_element_type=jnp.float32)
    return mixed, input_grad, gate_grad, up_grad, down_grad
```

```python
import jax
import jax.numpy as jnp
from jax import lax
from jax.sharding import PartitionSpec as P


def right_trans(left, matrix):
    return lax.dot_general(
        left, matrix, (((1,), (1,)), ((), ())), preferred_element_type=jnp.float32
    )


def left_trans(left, right):
    return lax.dot_general(
        left, right, (((0,), (0,)), ((), ())), preferred_element_type=jnp.float32
    )


def swap(x, step, n):
    return lax.ppermute(x, "dp", [(i, i ^ step) for i in range(n)])


def replicas(x, n):
    held = [(0, x)]
    step = n // 2
    while step:
        held += [(at ^ step, swap(piece, step, n)) for at, piece in held]
        step //= 2
    return [piece for _, piece in sorted(held, key=lambda p: p[0])]


def features(x, n):
    width = x.shape[1] // n
    own = lax.axis_index("dp")
    pieces = []
    for step in range(n):
        block = lax.dynamic_slice_in_dim(x, (own ^ step) * width, width, axis=1)
        pieces.append(swap(block, step, n) if step else block)
    return pieces


def make_body(n_dp):
    def body(tokens, w_gate, w_up, w_down, cotangent):
        gathered = lax.all_gather(tokens, "tp", axis=0, tiled=True)
        grad_full = lax.all_gather(cotangent, "tp", axis=0, tiled=True)
        token_pieces = features(gathered, n_dp)
        gate = jnp.dot(gathered, w_gate, preferred_element_type=jnp.float32)
        up = jnp.dot(gathered, w_up, preferred_element_type=jnp.float32)
        sig = jax.nn.sigmoid(gate)
        act = gate * sig
        hidden = (act * up).astype(jnp.bfloat16)
        hidden_pieces = replicas(hidden, n_dp)
        partial = jnp.dot(hidden, w_down, preferred_element_type=jnp.float32).astype(jnp.bfloat16)
        grad_full, partial, token_pieces, hidden_pieces = lax.optimization_barrier(
            (grad_full, partial, token_pieces, hidden_pieces)
        )
        mixed = lax.psum_scatter(partial, "tp", scatter_dimension=0, tiled=True)
        grad_pieces = features(grad_full, n_dp)
        back = right_trans(grad_full, w_down)
        dgate = (back * up * sig * (1.0 + gate * (1.0 - sig))).astype(jnp.bfloat16)
        dup = (back * act).astype(jnp.bfloat16)
        dgate_pieces = replicas(dgate, n_dp)
        dup_pieces = replicas(dup, n_dp)
        first = right_trans(dgate, w_gate)
        first, dup_here, grad_pieces = lax.optimization_barrier((first, dup, grad_pieces))
        input_grad = lax.psum_scatter(
            (first + right_trans(dup_here, w_up)).astype(jnp.bfloat16),
            "tp",
            scatter_dimension=0,
            tiled=True,
        )
        token_part = jnp.concatenate(token_pieces, axis=0)
        gate_grad = left_trans(token_part, jnp.concatenate(dgate_pieces, axis=0))
        up_grad = left_trans(token_part, jnp.concatenate(dup_pieces, axis=0))
        down_grad = left_trans(
            jnp.concatenate(hidden_pieces, axis=0), jnp.concatenate(grad_pieces, axis=0)
        )
        return (mixed, input_grad, gate_grad, up_grad, down_grad)

    return body


def solution(mesh):
    in_specs = (
        P(("dp", "tp"), None),
        P(None, "tp"),
        P(None, "tp"),
        P("tp", None),
        P(("dp", "tp"), None),
    )
    out_specs = (
        P(("dp", "tp"), None),
        P(("dp", "tp"), None),
        P("dp", "tp"),
        P("dp", "tp"),
        P("tp", "dp"),
    )
    body = make_body(mesh.shape["dp"])
    return jax.shard_map(body, mesh=mesh, in_specs=in_specs, out_specs=out_specs, check_vma=False)
```
